256 devices in a mesh: rp: 64 (over y, x, z_hi, core), re: 4 (over z_lo).
Axes of the slice: x: 4, y: 4, z: 8 (z_hi: 2, z_lo: 4; z = z_hi * 4 + z_lo), core: 2. Of those that a mesh axis runs over, the one named last changes fastest.
Arguments:
- coupling: bfloat16 [1024, 4, 2, 6, 4096], P('rp', 're'), may hold values from -0.4375 to 0.4375
- rp_coords: int32 [3, 1024], P(None, 'rp'), may hold values from -8 to 8
- degeneracy: int32 [1024], P('rp'), may hold values from 1 to 8
- qpoints: int32 [3, 512], replicated, may hold values from 0 to 15
- eigvec: float32 [512, 2, 6, 6], P('rp'), may hold values from -1.75 to 1.75
Outputs:
- coupling_q: float32 [512, 4, 2, 6, 4096], P('rp', None, None, None, 're')
The draws below stay inside these ranges and needn't reach their ends.
All inputs are finite; a program needn't handle non-finite values.
Results may differ from the reference program's by a relative error of at most 0.0042.
Values may be sent and summed in bfloat16 or wider, within the bound.
No kernel may reach another device: no remote copies, remote signals or barrier semaphores. Data moves between devices by JAX's collectives and lax.ppermute only.
A program may use at most 64 MiB of HBM per device.

```python
import math
import jax
import jax.numpy as jnp
from jax import lax

NW = 64
MODES = 6
QGRID = 16
RMAX = 8
RP = 1024
RE = 4
Q = 512


def plant(drawn, stream_key, smallest, top_value):
    longest = drawn.shape.index(max(drawn.shape))
    spots = []
    for shift in (0, 1):
        where = [jax.random.randint(jax.random.fold_in(stream_key, axis), (), 0, length) for axis, length in enumerate(drawn.shape)]
        where[longest] = (where[longest] + shift) % drawn.shape[longest]
        spots.append(tuple(where))
    return drawn.at[spots[0]].set(smallest).at[spots[1]].set(top_value)


def shard_levels(own_key, dims, pieces, low, top_value):
    gain = 1.0
    for dim, shards_of in pieces:
        steps = jax.random.uniform(jax.random.fold_in(jax.random.fold_in(own_key, 6), dim), (shards_of,), jnp.float32, low / len(pieces), top_value / len(pieces))
        gain = gain * jnp.repeat(jnp.exp(steps), dims[dim] // shards_of).reshape((-1,) + (1,) * (len(dims) - 1 - dim))
    return gain


def centred(rng, extent, width, bound, shards=(), dtype=jnp.bfloat16):
    result = width * jax.random.normal(rng, extent, jnp.float32)
    if shards:
        result = result * shard_levels(rng, extent, shards, -0.22, 0.18)
    return jnp.clip(result, -bound, bound).astype(dtype)


def setup_inputs(seed: int = 0) -> dict:
    streams_of = jax.random.split(jax.random.key(seed), 6)
    return {
        "coupling": centred(streams_of[0], (RP, RE, 2, MODES, NW * NW), (RP // 5) ** -0.5, 0.4375, ((0, 64), (1, 4))),
        "rp_coords": plant(jax.random.randint(streams_of[1], (3, RP), 0 - RMAX, RMAX + 1), jax.random.fold_in(streams_of[1], 1), 0 - RMAX, RMAX).astype(jnp.int32),
        "degeneracy": plant(jax.random.randint(streams_of[2], (RP,), 1, 9), jax.random.fold_in(streams_of[2], 1), 1, 8).astype(jnp.int32),
        "qpoints": plant(jax.random.randint(streams_of[3], (3, Q), 0, QGRID), jax.random.fold_in(streams_of[3], 1), 0, QGRID - 1).astype(jnp.int32),
        "eigvec": centred(streams_of[4], (Q, 2, MODES, MODES), (2 * MODES) ** -0.5, 1.75, ((0, 64),), jnp.float32),
    }


def phases(points, coords, degeneracy):
    turns = jnp.mod(points[0][:, None] * coords[0][None, :], QGRID)
    turns = turns + jnp.mod(points[1][:, None] * coords[1][None, :], QGRID)
    turns = turns + jnp.mod(points[2][:, None] * coords[2][None, :], QGRID)
    turns = jnp.mod(turns, QGRID)
    angles = turns.astype(jnp.float32) * (2.0 * math.pi / QGRID)
    weights = 1.0 / degeneracy.astype(jnp.float32)
    table = jnp.concatenate([jnp.cos(angles) * weights[None, :], jnp.sin(angles) * weights[None, :]], axis=0)
    return table.astype(jnp.bfloat16)


def combine(table, coupling):
    point_count = table.shape[0] // 2
    product = jnp.dot(table, coupling.reshape(coupling.shape[0], -1), preferred_element_type=jnp.float32)
    product = product.reshape((2, point_count) + coupling.shape[1:])
    real_part = product[0, :, :, 0] - product[1, :, :, 1]
    imag_part = product[0, :, :, 1] + product[1, :, :, 0]
    return jnp.stack([real_part, imag_part], axis=2)


def mode_mix(values, matrix):
    return jnp.einsum("qrkp,qkn->qrnp", values, matrix, precision=lax.Precision.HIGHEST)


def rotate(summed, eigvec):
    real_in = summed[:, :, 0]
    imag_in = summed[:, :, 1]
    vec_real = eigvec[:, 0]
    vec_imag = eigvec[:, 1]
    real_out = mode_mix(real_in, vec_real) - mode_mix(imag_in, vec_imag)
    imag_out = mode_mix(real_in, vec_imag) + mode_mix(imag_in, vec_real)
    return jnp.stack([real_out, imag_out], axis=2)


def reference(coupling, rp_coords, degeneracy, qpoints, eigvec):
    table = phases(qpoints, rp_coords, degeneracy)
    summed = combine(table, coupling)
    return rotate(summed, eigvec)
```

```python
import math

import jax
import jax.numpy as jnp
from jax import lax
from jax.experimental import pallas as pl
from jax.experimental.pallas import tpu as pltpu
from jax.sharding import Mesh, PartitionSpec as P

QGRID = 16
PLANE = ("y", "x", "core")
EVERY = ("y", "x", "zh", "core", "re")
DATA_ROWS = 192
ROWS = 200


def fetch_kernel(source, out, sems):
    for m in range(6):
        @pl.loop(0, 32)
        def _(b):
            pltpu.make_async_copy(
                source.at[:, m, :, pl.ds(pl.multiple_of(b * 128, 128), 128)],
                out.at[m, b],
                sems.at[m],
            ).start()
    for m in range(6):
        pltpu.make_async_copy(out.at[m], out.at[m], sems.at[m]).wait()


def fetch(coupling):
    return pl.pallas_call(
        fetch_kernel,
        out_shape=pltpu.VMEM((6, 32, 16, 2, 128), jnp.bfloat16),
        in_specs=[pl.BlockSpec(memory_space=pl.ANY)],
        out_specs=pl.BlockSpec(memory_space=pltpu.VMEM),
        scratch_shapes=[pltpu.SemaphoreType.DMA((6,))],
        name="fetch",
    )(coupling)


def pack_kernel(place, blocks, coords, degeneracy, out, lattice):
    lane = lax.broadcasted_iota(jnp.int32, (16, 128), 1)
    row = lax.broadcasted_iota(jnp.int32, (16, 128), 0)
    spread = (lane == place[0] * 32 + 2 * row) | (lane == place[0] * 32 + 2 * row + 1)
    spread = spread.astype(jnp.float32).astype(jnp.bfloat16)
    lattice[...] = jnp.zeros_like(lattice)
    lattice[0:3, :] = jnp.dot(
        coords[...].astype(jnp.float32).astype(jnp.bfloat16), spread, preferred_element_type=jnp.float32
    )
    lattice[3:4, :] = jnp.dot(
        degeneracy[...].astype(jnp.float32).astype(jnp.bfloat16), spread, preferred_element_type=jnp.float32
    )
    mine = lattice[...].astype(jnp.bfloat16)

    @pl.loop(0, 8)
    def _(pair):
        for m in range(6):
            for half in range(2):
                a = blocks[m, 16 * half + pair]
                b = blocks[m, 16 * half + 8 + pair]
                at = pl.ds((m % 3 * 2 + half) * 32, 32)
                out[4 * pair + m // 3, at, :] = jnp.concatenate([a[:, :64], b[:, :64]], axis=1)
                out[4 * pair + 2 + m // 3, at, :] = jnp.concatenate([a[:, 64:], b[:, 64:]], axis=1)
        for u in range(4):
            out[4 * pair + u, DATA_ROWS:ROWS, :] = mine


def pack(place, blocks, coords, degeneracy):
    vmem = pl.BlockSpec(memory_space=pltpu.VMEM)
    return pl.pallas_call(
        pack_kernel,
        out_shape=pltpu.VMEM((32, ROWS, 128), jnp.bfloat16),
        in_specs=[pl.BlockSpec(memory_space=pltpu.SMEM), vmem, vmem, vmem],
        out_specs=vmem,
        scratch_shapes=[pltpu.VMEM((8, 128), jnp.float32)],
        name="pack",
    )(place, blocks, coords, degeneracy)


def combine_kernel(received, points, out, table):
    lane = lax.broadcasted_iota(jnp.int32, (512, 128), 1)
    odd = lane & 1
    position = lax.broadcasted_iota(jnp.int32, (1, 128), 1)
    cosines = jnp.zeros((1, 128), jnp.float32)
    for i in range(QGRID):
        value = math.cos(2.0 * math.pi * i / QGRID) if i % 8 != 4 else 0.0
        cosines = jnp.where(position == i, value, cosines)
    cosines = jnp.broadcast_to(cosines, (512, 128))
    q = points[...].astype(jnp.bfloat16)

    @pl.loop(0, 8)
    def _(k):
        rows = received[pl.ds(4 * k, 4), DATA_ROWS:ROWS, :].astype(jnp.float32)
        rows = rows[0] + rows[1] + rows[2] + rows[3]
        weights = 1.0 / rows[3:4, :]
        turns = jnp.dot(q, rows.astype(jnp.bfloat16), preferred_element_type=jnp.float32).astype(jnp.int32)
        first = jnp.take_along_axis(cosines, (turns + 4 * odd) & (QGRID - 1), axis=1)
        second = jnp.take_along_axis(cosines, (turns + 12 - 12 * odd) & (QGRID - 1), axis=1)
        at = pl.ds(pl.multiple_of(k * 128, 128), 128)
        table[0:512, at] = (first * weights).astype(jnp.bfloat16)
        table[512:1024, at] = (second * weights).astype(jnp.bfloat16)

    low = lax.broadcasted_iota(jnp.int32, (512, 128), 1) < 64

    @pl.loop(0, 3)
    def _(m):
        at = pl.multiple_of(m * 64, 64)
        columns = jnp.concatenate(
            [
                received[:, pl.ds(at, 32), :].reshape(1024, 128),
                received[:, pl.ds(at + 32, 32), :].reshape(1024, 128),
            ],
            axis=1,
        )
        product = jnp.dot(table[...], columns, preferred_element_type=jnp.float32)
        rows = pl.ds(pl.multiple_of(m * 8, 8), 8)
        for half in range(2):
            real = product[0:512, 128 * half : 128 * half + 128]
            imag = product[512:1024, 128 * half : 128 * half + 128]
            near = jnp.where(low, real, pltpu.roll(imag, 64, 1))
            far = jnp.where(low, pltpu.roll(real, 64, 1), imag)
            out[:, 2 * half, rows, :] = near.reshape(64, 8, 128).astype(jnp.bfloat16)
            out[:, 2 * half + 1, rows, :] = far.reshape(64, 8, 128).astype(jnp.bfloat16)


def combine(received, points):
    vmem = pl.BlockSpec(memory_space=pltpu.VMEM)
    return pl.pallas_call(
        combine_kernel,
        out_shape=pltpu.VMEM((64, 4, 24, 128), jnp.bfloat16),
        in_specs=[vmem, vmem],
        out_specs=vmem,
        scratch_shapes=[pltpu.VMEM((1024, 1024), jnp.bfloat16)],
        name="combine",
    )(received, points)


def rotate_kernel(summed, eigvec, out, factors):
    for i in range(72):
        factors[i] = jnp.broadcast_to(eigvec[:, i : i + 1], (8, 128))
    low = lax.broadcasted_iota(jnp.int32, (8, 128), 1) < 64

    @pl.loop(0, 32)
    def _(step):
        e = step // 8
        block = step % 8

        def piece(h, k):
            rows = pl.ds(k % 3 * 8, 8)
            return summed[2 * block + h, 0, k // 3, e, rows, :].astype(jnp.float32) + summed[
                2 * block + h, 1, k // 3, e, rows, :
            ].astype(jnp.float32)

        real, imag = [], []
        for k in range(6):
            left, right = piece(0, k), piece(1, k)
            real.append(jnp.where(low, left, pltpu.roll(right, 64, 1)))
            imag.append(jnp.where(low, pltpu.roll(left, 64, 1), right))
        for n in range(6):
            real_out = jnp.zeros((8, 128), jnp.float32)
            imag_out = jnp.zeros((8, 128), jnp.float32)
            for k in range(6):
                vec_real = factors[k * 6 + n]
                vec_imag = factors[36 + k * 6 + n]
                real_out = real_out + real[k] * vec_real - imag[k] * vec_imag
                imag_out = imag_out + real[k] * vec_imag + imag[k] * vec_real
            at = e * 96 + n * 16 + block * 2
            out[pl.ds(at, 8, stride=384), :] = real_out
            out[pl.ds(at + 1, 8, stride=384), :] = imag_out


def rotate(summed, eigvec):
    vmem = pl.BlockSpec(memory_space=pltpu.VMEM)
    return pl.pallas_call(
        rotate_kernel,
        out_shape=jax.ShapeDtypeStruct((3072, 128), jnp.float32),
        in_specs=[vmem, vmem],
        out_specs=vmem,
        scratch_shapes=[pltpu.VMEM((72, 8, 128), jnp.float32)],
        name="rotate",
    )(summed, eigvec)


def per_device(coupling, rp_coords, degeneracy, qpoints, eigvec):
    place = (lax.axis_index(PLANE) % 4).astype(jnp.int32).reshape(1)
    points = jnp.pad(qpoints.T.astype(jnp.float32), ((0, 0), (0, 5)))
    vectors = eigvec.reshape(8, 72)
    blocks = fetch(coupling.reshape(16, 2, 6, 4096).transpose(0, 2, 1, 3)).reshape(6, 32, 32, 128)
    message = pack(place, blocks, rp_coords, degeneracy.reshape(1, 16))
    received = lax.all_to_all(message, PLANE, 0, 0, tiled=True)
    partial = combine(received, points).reshape(256, 24, 128)
    summed = lax.all_to_all(partial, EVERY, 0, 0, tiled=True)
    result = rotate(summed.reshape(16, 2, 2, 4, 24, 128), vectors)
    return result.reshape(8, 4, 6, 8, 2, 128).transpose(0, 1, 4, 2, 3, 5).reshape(8, 4, 2, 6, 1024)


def solution(mesh):
    rp = ("y", "x", "zh", "core")
    inner = Mesh(mesh.devices.reshape(4, 4, 2, 2, 4), EVERY)
    return jax.shard_map(
        per_device,
        mesh=inner,
        in_specs=(P(rp, "re", None, None, None), P(None, rp), P(rp), P(), P(rp, None, None, None)),
        out_specs=P(rp, None, None, None, "re"),
        check_vma=False,
    )
```

```python
import math

import jax
import jax.numpy as jnp
from jax import lax
from jax.experimental import pallas as pl
from jax.experimental.pallas import tpu as pltpu
from jax.sharding import Mesh, PartitionSpec as P

QGRID = 16
PLANE = ("y", "x", "core")
EVERY = ("y", "x", "zh", "core", "re")
DATA_ROWS = 192
ROWS = 200


def fetch_kernel(source, out, sems):
    for m in range(6):
        @pl.loop(0, 32, unroll=8)
        def _(b):
            pltpu.make_async_copy(
                source.at[:, m, :, pl.ds(pl.multiple_of(b * 128, 128), 128)],
                out.at[m, b],
                sems.at[m],
            ).start()
    for m in range(6):
        pltpu.make_async_copy(out.at[m], out.at[m], sems.at[m]).wait()


def fetch(coupling):
    return pl.pallas_call(
        fetch_kernel,
        out_shape=pltpu.VMEM((6, 32, 16, 2, 128), jnp.bfloat16),
        in_specs=[pl.BlockSpec(memory_space=pl.ANY)],
        out_specs=pl.BlockSpec(memory_space=pltpu.VMEM),
        scratch_shapes=[pltpu.SemaphoreType.DMA((6,))],
        name="fetch",
    )(coupling)


def pack_kernel(place, blocks, coords, degeneracy, out, lattice):
    lane = lax.broadcasted_iota(jnp.int32, (16, 128), 1)
    row = lax.broadcasted_iota(jnp.int32, (16, 128), 0)
    spread = (lane == place[0] * 32 + 2 * row) | (lane == place[0] * 32 + 2 * row + 1)
    spread = spread.astype(jnp.float32).astype(jnp.bfloat16)
    lattice[...] = jnp.zeros_like(lattice)
    lattice[0:3, :] = jnp.dot(
        coords[...].astype(jnp.float32).astype(jnp.bfloat16), spread, preferred_element_type=jnp.float32
    )
    lattice[3:4, :] = jnp.dot(
        degeneracy[...].astype(jnp.float32).astype(jnp.bfloat16), spread, preferred_element_type=jnp.float32
    )
    mine = lattice[...].astype(jnp.bfloat16)

    @pl.loop(0, 8, unroll=2)
    def _(pair):
        for m in range(6):
            for half in range(2):
                a = blocks[m, 16 * half + pair]
                b = blocks[m, 16 * half + 8 + pair]
                at = pl.ds((m % 3 * 2 + half) * 32, 32)
                out[4 * pair + m // 3, at, :] = jnp.concatenate([a[:, :64], b[:, :64]], axis=1)
                out[4 * pair + 2 + m // 3, at, :] = jnp.concatenate([a[:, 64:], b[:, 64:]], axis=1)
        for u in range(4):
            out[4 * pair + u, DATA_ROWS:ROWS, :] = mine


def pack(place, blocks, coords, degeneracy):
    vmem = pl.BlockSpec(memory_space=pltpu.VMEM)
    return pl.pallas_call(
        pack_kernel,
        out_shape=pltpu.VMEM((32, ROWS, 128), jnp.bfloat16),
        in_specs=[pl.BlockSpec(memory_space=pltpu.SMEM), vmem, vmem, vmem],
        out_specs=vmem,
        scratch_shapes=[pltpu.VMEM((8, 128), jnp.float32)],
        name="pack",
    )(place, blocks, coords, degeneracy)


def combine_kernel(received, points, out, table, lattice):
    shift = 4.0 * (lax.broadcasted_iota(jnp.int32, (1, 128), 1) & 1).astype(jnp.float32)
    for k in range(8):
        at = slice(k * 128, k * 128 + 128)
        rows = received[4 * k : 4 * k + 4, DATA_ROWS:ROWS, :].astype(jnp.float32)
        rows = rows[0] + rows[1] + rows[2] + rows[3]
        lattice[0:3, at] = rows[0:3]
        lattice[3:4, at] = 1.0 / rows[3:4]
    c1, c2, c3 = (math.cos(2.0 * math.pi * i / QGRID) for i in (1, 2, 3))

    @pl.loop(0, 16)
    def _(chunk):
        q = points[pl.ds(pl.multiple_of(chunk * 32, 32), 32), :]
        q0, q1, q2 = (jnp.broadcast_to(q[:, d : d + 1], (32, 128)) for d in range(3))
        for k in range(8):
            at = slice(k * 128, k * 128 + 128)
            turns = q0 * lattice[0:1, at] + q1 * lattice[1:2, at] + (q2 * lattice[2:3, at] + shift)
            turns = turns.astype(jnp.int32)
            bit0, bit1, bit2, bit3 = ((turns & b) != 0 for b in (1, 2, 4, 8))
            cosine = jnp.where(bit1, jnp.where(bit0, c3, c2), jnp.where(bit0, c1, 1.0))
            sine = jnp.where(bit1, jnp.where(bit0, c1, c2), jnp.where(bit0, c3, 0.0))
            weight = jnp.broadcast_to(lattice[3:4, at], (32, 128))
            sine_weight = jnp.where(bit3, -weight, weight)
            cosine_weight = jnp.where(bit2, -sine_weight, sine_weight)
            first = jnp.where(bit2, sine, cosine) * cosine_weight
            second = jnp.where(bit2, cosine, sine) * sine_weight
            table[pl.ds(pl.multiple_of(chunk * 32, 32), 32), at] = first.astype(jnp.bfloat16)
            table[pl.ds(pl.multiple_of(512 + chunk * 32, 32), 32), at] = second.astype(jnp.bfloat16)

    low = lax.broadcasted_iota(jnp.int32, (512, 128), 1) < 64

    @pl.loop(0, 3)
    def _(m):
        at = pl.multiple_of(m * 64, 64)
        columns = jnp.concatenate(
            [
                received[:, pl.ds(at, 32), :].reshape(1024, 128),
                received[:, pl.ds(at + 32, 32), :].reshape(1024, 128),
            ],
            axis=1,
        )
        product = jnp.dot(table[...], columns, preferred_element_type=jnp.float32)
        rows = pl.ds(pl.multiple_of(m * 8, 8), 8)
        for half in range(2):
            real = product[0:512, 128 * half : 128 * half + 128]
            imag = product[512:1024, 128 * half : 128 * half + 128]
            near = jnp.where(low, real, pltpu.roll(imag, 64, 1))
            far = jnp.where(low, pltpu.roll(real, 64, 1), imag)
            out[:, 2 * half, rows, :] = near.reshape(64, 8, 128).astype(jnp.bfloat16)
            out[:, 2 * half + 1, rows, :] = far.reshape(64, 8, 128).astype(jnp.bfloat16)


def combine(received, points):
    vmem = pl.BlockSpec(memory_space=pltpu.VMEM)
    return pl.pallas_call(
        combine_kernel,
        out_shape=pltpu.VMEM((64, 4, 24, 128), jnp.bfloat16),
        in_specs=[vmem, vmem],
        out_specs=vmem,
        scratch_shapes=[pltpu.VMEM((1024, 1024), jnp.bfloat16), pltpu.VMEM((8, 1024), jnp.float32)],
        name="combine",
    )(received, points)


def rotate_kernel(summed, eigvec, out, factors, result, sem):
    for i in range(72):
        factors[i] = jnp.broadcast_to(eigvec[:, i : i + 1], (8, 128))
    low = lax.broadcasted_iota(jnp.int32, (8, 128), 1) < 64

    @pl.loop(0, 4)
    def _(e):
        def piece(h, k):
            rows = slice(k % 3 * 8, k % 3 * 8 + 8)
            return summed[h, 0, k // 3, e, rows, :].astype(jnp.float32) + summed[
                h, 1, k // 3, e, rows, :
            ].astype(jnp.float32)

        @pl.loop(0, 4, unroll=4)
        def _(step):
            blocks = (2 * step, 2 * step + 1)
            real, imag = {}, {}
            for i, block in enumerate(blocks):
                for k in range(6):
                    left, right = piece(2 * block, k), piece(2 * block + 1, k)
                    real[i, k] = jnp.where(low, left, pltpu.roll(right, 64, 1))
                    imag[i, k] = jnp.where(low, pltpu.roll(left, 64, 1), right)
            for n in range(6):
                totals = {}
                for k in range(6):
                    vec_real = factors[k * 6 + n]
                    vec_imag = factors[36 + k * 6 + n]
                    for i in range(2):
                        terms = (
                            real[i, k] * vec_real - imag[i, k] * vec_imag,
                            real[i, k] * vec_imag + imag[i, k] * vec_real,
                        )
                        for part in range(2):
                            totals[i, part] = totals[i, part] + terms[part] if k else terms[part]
                for i, block in enumerate(blocks):
                    for part in range(2):
                        at = e * 96 + n * 16 + block * 2 + part
                        result[pl.ds(at, 8, stride=384), :] = totals[i, part]

        for q in range(8):
            at = pl.ds(pl.multiple_of(q * 384 + e * 96, 32), 96)
            pltpu.make_async_copy(result.at[at], out.at[at], sem).start()

    pltpu.make_async_copy(result, out, sem).wait()


def rotate(summed, eigvec):
    vmem = pl.BlockSpec(memory_space=pltpu.VMEM)
    return pl.pallas_call(
        rotate_kernel,
        out_shape=jax.ShapeDtypeStruct((3072, 128), jnp.float32),
        in_specs=[vmem, vmem],
        out_specs=pl.BlockSpec(memory_space=pl.ANY),
        scratch_shapes=[
            pltpu.VMEM((72, 8, 128), jnp.float32),
            pltpu.VMEM((3072, 128), jnp.float32),
            pltpu.SemaphoreType.DMA,
        ],
        name="rotate",
    )(summed, eigvec)


def on_chip(x):
    return pltpu.with_memory_space_constraint(x, pltpu.VMEM)


def per_device(coupling, rp_coords, degeneracy, qpoints, eigvec):
    place = (lax.axis_index(PLANE) % 4).astype(jnp.int32).reshape(1)
    points = jnp.pad(qpoints.T.astype(jnp.float32), ((0, 0), (0, 5)))
    vectors = eigvec.reshape(8, 72)
    blocks = fetch(coupling.reshape(16, 2, 6, 4096).transpose(0, 2, 1, 3)).reshape(6, 32, 32, 128)
    message = pack(place, on_chip(blocks), rp_coords, degeneracy.reshape(1, 16))
    received = lax.all_to_all(message, PLANE, 0, 0, tiled=True)
    partial = combine(on_chip(received), points).reshape(256, 24, 128)
    summed = lax.all_to_all(partial, EVERY, 0, 0, tiled=True)
    result = rotate(on_chip(summed.reshape(16, 2, 2, 4, 24, 128)), vectors)
    return result.reshape(8, 4, 6, 8, 2, 128).transpose(0, 1, 4, 2, 3, 5).reshape(8, 4, 2, 6, 1024)


def solution(mesh):
    rp = ("y", "x", "zh", "core")
    inner = Mesh(mesh.devices.reshape(4, 4, 2, 2, 4), EVERY)
    return jax.shard_map(
        per_device,
        mesh=inner,
        in_specs=(P(rp, "re", None, None, None), P(None, rp), P(rp), P(), P(rp, None, None, None)),
        out_specs=P(rp, None, None, None, "re"),
        check_vma=False,
    )
```

```python
import math

import jax
import jax.numpy as jnp
from jax import lax
from jax.experimental import pallas as pl
from jax.experimental.pallas import tpu as pltpu
from jax.sharding import Mesh, PartitionSpec as P

QGRID = 16
PLANE = ("y", "x", "core")
EVERY = ("y", "x", "zh", "core", "re")
DATA_ROWS = 192
ROWS = 200


def fetch_kernel(
    place, coupling, coords, degeneracy, qpoints, eigvec,
    blocks, mine, points, factors,
    coords_in, degeneracy_in, qpoints_in, eigvec_in, rows, columns, sems, small_sems,
):
    small = [
        pltpu.make_async_copy(source, target, small_sems.at[i])
        for i, (source, target) in enumerate(
            [(coords, coords_in), (degeneracy, degeneracy_in), (qpoints, qpoints_in), (eigvec, eigvec_in)]
        )
    ]
    for copy in small:
        copy.start()
    for m in range(6):
        @pl.loop(0, 32, unroll=8)
        def _(b):
            pltpu.make_async_copy(
                coupling.at[:, m, :, pl.ds(pl.multiple_of(b * 128, 128), 128)],
                blocks.at[m, b],
                sems.at[m],
            ).start()
    for copy in small:
        copy.wait()

    lane = lax.broadcasted_iota(jnp.int32, (16, 128), 1)
    row = lax.broadcasted_iota(jnp.int32, (16, 128), 0)
    spread = (lane == place[0] * 32 + 2 * row) | (lane == place[0] * 32 + 2 * row + 1)
    spread = spread.astype(jnp.float32).astype(jnp.bfloat16)
    rows[...] = jnp.zeros_like(rows)
    for at, values in ((slice(0, 3), coords_in), (slice(3, 4), degeneracy_in)):
        rows[at, 0:128] = jnp.dot(
            values[...].astype(jnp.float32).astype(jnp.bfloat16), spread, preferred_element_type=jnp.float32
        )
    mine[...] = rows[:, 0:128].astype(jnp.bfloat16)

    rows[...] = jnp.zeros_like(rows)
    rows[0:3, :] = qpoints_in[...].astype(jnp.float32)
    points[...] = jnp.transpose(rows[...])

    columns[...] = jnp.zeros_like(columns)
    for part in range(2):
        for k in range(6):
            for n in range(6):
                i = part * 36 + k * 6 + n
                columns[i : i + 1, 0:8] = eigvec_in[k, n, part : part + 1, :]
    turned = jnp.transpose(columns[...])
    for i in range(72):
        factors[i] = jnp.broadcast_to(turned[0:8, i : i + 1], (8, 128))

    for m in range(6):
        pltpu.make_async_copy(blocks.at[m], blocks.at[m], sems.at[m]).wait()


VMEM = pl.BlockSpec(memory_space=pltpu.VMEM)
LIMIT = 16 * 2**20


def on_chip(x):
    return pltpu.with_memory_space_constraint(x, pltpu.VMEM)


def fetch(place, coupling, coords, degeneracy, qpoints, eigvec):
    hbm = pl.BlockSpec(memory_space=pltpu.HBM)
    return pl.pallas_call(
        fetch_kernel,
        out_shape=(
            pltpu.VMEM((6, 32, 16, 2, 128), jnp.bfloat16),
            pltpu.VMEM((8, 128), jnp.bfloat16),
            pltpu.VMEM((512, 8), jnp.float32),
            pltpu.VMEM((72, 8, 128), jnp.float32),
        ),
        in_specs=[pl.BlockSpec(memory_space=pltpu.SMEM)] + [hbm] * 5,
        out_specs=(VMEM,) * 4,
        scratch_shapes=[
            pltpu.VMEM((3, 16), jnp.int32),
            pltpu.VMEM((1, 16), jnp.int32),
            pltpu.VMEM((3, 512), jnp.int32),
            pltpu.VMEM((6, 6, 2, 8), jnp.float32),
            pltpu.VMEM((8, 512), jnp.float32),
            pltpu.VMEM((128, 128), jnp.float32),
            pltpu.SemaphoreType.DMA((6,)),
            pltpu.SemaphoreType.DMA((4,)),
        ],
        compiler_params=pltpu.CompilerParams(vmem_limit_bytes=LIMIT),
        name="fetch",
    )(place, *(pltpu.with_memory_space_constraint(x, pltpu.HBM) for x in (coupling, coords, degeneracy, qpoints, eigvec)))


def pack_kernel(blocks, mine, out):
    @pl.loop(0, 8, unroll=2)
    def _(pair):
        for m in range(6):
            for half in range(2):
                a = blocks[m, 16 * half + pair]
                b = blocks[m, 16 * half + 8 + pair]
                at = pl.ds((m % 3 * 2 + half) * 32, 32)
                out[4 * pair + m // 3, at, :] = jnp.concatenate([a[:, :64], b[:, :64]], axis=1)
                out[4 * pair + 2 + m // 3, at, :] = jnp.concatenate([a[:, 64:], b[:, 64:]], axis=1)
        for u in range(4):
            out[4 * pair + u, DATA_ROWS:ROWS, :] = mine[...]


def pack(blocks, mine):
    return pl.pallas_call(
        pack_kernel,
        out_shape=pltpu.VMEM((32, ROWS, 128), jnp.bfloat16),
        in_specs=[VMEM] * 2,
        out_specs=VMEM,
        compiler_params=pltpu.CompilerParams(vmem_limit_bytes=LIMIT),
        name="pack",
    )(on_chip(blocks), on_chip(mine))


CHUNK = 128


def combine_kernel(received, points, out, lattice, *tables):
    shift = 4.0 * (lax.broadcasted_iota(jnp.int32, (1, 128), 1) & 1).astype(jnp.float32)
    for k in range(8):
        at = slice(k * 128, k * 128 + 128)
        rows = received[4 * k : 4 * k + 4, DATA_ROWS:ROWS, :].astype(jnp.float32)
        rows = rows[0] + rows[1] + rows[2] + rows[3]
        lattice[0:3, at] = rows[0:3]
        lattice[3:4, at] = 1.0 / rows[3:4]
    c1, c2, c3 = (math.cos(2.0 * math.pi * i / QGRID) for i in (1, 2, 3))
    low = lax.broadcasted_iota(jnp.int32, (CHUNK, 128), 1) < 64

    for c, table in enumerate(tables):
        for piece in range(CHUNK // 32):
            q = points[c * CHUNK + piece * 32 : c * CHUNK + piece * 32 + 32, :]
            q0, q1, q2 = (jnp.broadcast_to(q[:, d : d + 1], (32, 128)) for d in range(3))
            for k in range(8):
                at = slice(k * 128, k * 128 + 128)
                turns = q0 * lattice[0:1, at] + q1 * lattice[1:2, at] + (q2 * lattice[2:3, at] + shift)
                turns = turns.astype(jnp.int32)
                bit0, bit1, bit2, bit3 = ((turns & b) != 0 for b in (1, 2, 4, 8))
                cosine = jnp.where(bit1, jnp.where(bit0, c3, c2), jnp.where(bit0, c1, 1.0))
                sine = jnp.where(bit1, jnp.where(bit0, c1, c2), jnp.where(bit0, c3, 0.0))
                weight = jnp.broadcast_to(lattice[3:4, at], (32, 128))
                sine_weight = jnp.where(bit3, -weight, weight)
                cosine_weight = jnp.where(bit2, -sine_weight, sine_weight)
                first = jnp.where(bit2, sine, cosine) * cosine_weight
                second = jnp.where(bit2, cosine, sine) * sine_weight
                table[piece * 32 : piece * 32 + 32, at] = first.astype(jnp.bfloat16)
                table[CHUNK + piece * 32 : CHUNK + piece * 32 + 32, at] = second.astype(jnp.bfloat16)

        owners = slice(c * CHUNK // 8, (c + 1) * CHUNK // 8)
        for m in range(3):
            columns = jnp.concatenate(
                [
                    received[:, m * 64 : m * 64 + 32, :].reshape(1024, 128),
                    received[:, m * 64 + 32 : m * 64 + 64, :].reshape(1024, 128),
                ],
                axis=1,
            )
            product = jnp.dot(table[...], columns, preferred_element_type=jnp.float32)
            rows = slice(m * 8, m * 8 + 8)
            for half in range(2):
                real = product[:CHUNK, 128 * half : 128 * half + 128]
                imag = product[CHUNK:, 128 * half : 128 * half + 128]
                near = jnp.where(low, real, pltpu.roll(imag, 64, 1))
                far = jnp.where(low, pltpu.roll(real, 64, 1), imag)
                out[owners, 2 * half, rows, :] = near.reshape(CHUNK // 8, 8, 128).astype(jnp.bfloat16)
                out[owners, 2 * half + 1, rows, :] = far.reshape(CHUNK // 8, 8, 128).astype(jnp.bfloat16)


def combine(received, points):
    return pl.pallas_call(
        combine_kernel,
        out_shape=pltpu.VMEM((64, 4, 24, 128), jnp.bfloat16),
        in_specs=[VMEM] * 2,
        out_specs=VMEM,
        scratch_shapes=[pltpu.VMEM((8, 1024), jnp.float32)]
        + [pltpu.VMEM((2 * CHUNK, 1024), jnp.bfloat16)] * (512 // CHUNK),
        compiler_params=pltpu.CompilerParams(vmem_limit_bytes=LIMIT),
        name="combine",
    )(on_chip(received), on_chip(points))


def rotate_kernel(summed, factors, out, result, sem):
    low = lax.broadcasted_iota(jnp.int32, (8, 128), 1) < 64

    @pl.loop(0, 4)
    def _(e):
        def piece(h, k):
            rows = slice(k % 3 * 8, k % 3 * 8 + 8)
            return summed[h, 0, k // 3, e, rows, :].astype(jnp.float32) + summed[
                h, 1, k // 3, e, rows, :
            ].astype(jnp.float32)

        @pl.loop(0, 4, unroll=4)
        def _(step):
            blocks = (2 * step, 2 * step + 1)
            real, imag = {}, {}
            for i, block in enumerate(blocks):
                for k in range(6):
                    left, right = piece(2 * block, k), piece(2 * block + 1, k)
                    real[i, k] = jnp.where(low, left, pltpu.roll(right, 64, 1))
                    imag[i, k] = jnp.where(low, pltpu.roll(left, 64, 1), right)
            for n in range(6):
                totals = {}
                for k in range(6):
                    vec_real = factors[k * 6 + n]
                    vec_imag = factors[36 + k * 6 + n]
                    for i in range(2):
                        terms = (
                            real[i, k] * vec_real - imag[i, k] * vec_imag,
                            real[i, k] * vec_imag + imag[i, k] * vec_real,
                        )
                        for part in range(2):
                            totals[i, part] = totals[i, part] + terms[part] if k else terms[part]
                for i, block in enumerate(blocks):
                    for part in range(2):
                        at = e * 96 + n * 16 + block * 2 + part
                        result[pl.ds(at, 8, stride=384), :] = totals[i, part]

        for q in range(8):
            at = pl.ds(pl.multiple_of(q * 384 + e * 96, 32), 96)
            pltpu.make_async_copy(result.at[at], out.at[at], sem).start()

    pltpu.make_async_copy(result, out, sem).wait()


def rotate(summed, factors):
    return pl.pallas_call(
        rotate_kernel,
        out_shape=jax.ShapeDtypeStruct((3072, 128), jnp.float32),
        in_specs=[VMEM] * 2,
        out_specs=pl.BlockSpec(memory_space=pltpu.HBM),
        scratch_shapes=[pltpu.VMEM((3072, 128), jnp.float32), pltpu.SemaphoreType.DMA],
        compiler_params=pltpu.CompilerParams(vmem_limit_bytes=LIMIT),
        name="rotate",
    )(on_chip(summed), on_chip(factors))


def per_device(coupling, rp_coords, degeneracy, qpoints, eigvec):
    place = (lax.axis_index(PLANE) % 4).astype(jnp.int32).reshape(1)
    blocks, mine, points, factors = fetch(
        place,
        coupling.reshape(16, 2, 6, 4096).transpose(0, 2, 1, 3),
        rp_coords,
        degeneracy.reshape(1, 16),
        qpoints,
        eigvec.transpose(2, 3, 1, 0),
    )
    message = pack(blocks.reshape(6, 32, 32, 128), mine)
    received = lax.all_to_all(message, PLANE, 0, 0, tiled=True)
    partial = combine(received, points).reshape(256, 24, 128)
    summed = lax.all_to_all(partial, EVERY, 0, 0, tiled=True)
    result = rotate(summed.reshape(16, 2, 2, 4, 24, 128), factors)
    return result.reshape(8, 4, 6, 8, 2, 128).transpose(0, 1, 4, 2, 3, 5).reshape(8, 4, 2, 6, 1024)


def solution(mesh):
    rp = ("y", "x", "zh", "core")
    inner = Mesh(mesh.devices.reshape(4, 4, 2, 2, 4), EVERY)
    return jax.shard_map(
        per_device,
        mesh=inner,
        in_specs=(P(rp, "re", None, None, None), P(None, rp), P(rp), P(), P(rp, None, None, None)),
        out_specs=P(rp, None, None, None, "re"),
        check_vma=False,
    )
```

```python
import math

import jax
import jax.numpy as jnp
from jax import lax
from jax.experimental import pallas as pl
from jax.experimental.pallas import tpu as pltpu
from jax.sharding import Mesh, PartitionSpec as P

QGRID = 16
PLANE = ("y", "x", "core")
EVERY = ("y", "x", "zh", "core", "re")
DATA_ROWS = 192
ROWS = 200


def fetch_kernel(
    place, coupling, coords, degeneracy, qpoints, eigvec,
    blocks, mine, points, factors,
    coords_in, degeneracy_in, qpoints_in, eigvec_in, rows, columns, sems, small_sems,
):
    small = [
        pltpu.make_async_copy(source, target, small_sems.at[i])
        for i, (source, target) in enumerate(
            [(coords, coords_in), (degeneracy, degeneracy_in), (qpoints, qpoints_in), (eigvec, eigvec_in)]
        )
    ]
    for copy in small:
        copy.start()
    for m in range(6):
        @pl.loop(0, 4)
        def _(group):
            for i in range(8):
                b = group * 8 + i
                pltpu.make_async_copy(
                    coupling.at[:, m, :, pl.ds(pl.multiple_of(b * 128, 128), 128)],
                    blocks.at[m, b],
                    sems.at[m],
                ).start(priority=i % 2)
    for copy in small:
        copy.wait()

    lane = lax.broadcasted_iota(jnp.int32, (16, 128), 1)
    row = lax.broadcasted_iota(jnp.int32, (16, 128), 0)
    spread = (lane == place[0] * 16 + row).astype(jnp.float32).astype(jnp.bfloat16)
    rows[...] = jnp.zeros_like(rows)
    for at, values in ((slice(0, 3), coords_in), (slice(3, 4), degeneracy_in)):
        rows[at, 0:128] = jnp.dot(
            values[...].astype(jnp.float32).astype(jnp.bfloat16), spread, preferred_element_type=jnp.float32
        )
    mine[...] = rows[:, 0:128].astype(jnp.bfloat16)

    rows[...] = jnp.zeros_like(rows)
    rows[0:3, :] = qpoints_in[...].astype(jnp.float32)
    points[...] = jnp.transpose(rows[...])

    columns[...] = jnp.zeros_like(columns)
    for part in range(2):
        for k in range(6):
            for n in range(6):
                i = part * 36 + k * 6 + n
                columns[i : i + 1, 0:8] = eigvec_in[k, n, part : part + 1, :]
    turned = jnp.transpose(columns[...])
    for i in range(72):
        factors[i] = jnp.broadcast_to(turned[0:8, i : i + 1], (8, 128))

    for m in range(6):
        pltpu.make_async_copy(blocks.at[m], blocks.at[m], sems.at[m]).wait()


VMEM = pl.BlockSpec(memory_space=pltpu.VMEM)
LIMIT = 16 * 2**20


def on_chip(x):
    return pltpu.with_memory_space_constraint(x, pltpu.VMEM)


def fetch(place, coupling, coords, degeneracy, qpoints, eigvec):
    hbm = pl.BlockSpec(memory_space=pltpu.HBM)
    return pl.pallas_call(
        fetch_kernel,
        out_shape=(
            pltpu.VMEM((6, 32, 16, 2, 128), jnp.bfloat16),
            pltpu.VMEM((8, 128), jnp.bfloat16),
            pltpu.VMEM((512, 8), jnp.float32),
            pltpu.VMEM((72, 8, 128), jnp.float32),
        ),
        in_specs=[pl.BlockSpec(memory_space=pltpu.SMEM)] + [hbm] * 5,
        out_specs=(VMEM,) * 4,
        scratch_shapes=[
            pltpu.VMEM((3, 16), jnp.int32),
            pltpu.VMEM((1, 16), jnp.int32),
            pltpu.VMEM((3, 512), jnp.int32),
            pltpu.VMEM((6, 6, 2, 8), jnp.float32),
            pltpu.VMEM((8, 512), jnp.float32),
            pltpu.VMEM((128, 128), jnp.float32),
            pltpu.SemaphoreType.DMA((6,)),
            pltpu.SemaphoreType.DMA((4,)),
        ],
        compiler_params=pltpu.CompilerParams(vmem_limit_bytes=LIMIT),
        name="fetch",
    )(place, *(pltpu.with_memory_space_constraint(x, pltpu.HBM) for x in (coupling, coords, degeneracy, qpoints, eigvec)))


SLOTS = 8


def pack_kernel(blocks, mine, out, halves):
    @pl.loop(0, 8, unroll=2)
    def _(pair):
        slot = 0
        for m in range(6):
            for half in range(2):
                a = blocks[m, 16 * half + pair]
                b = blocks[m, 16 * half + 8 + pair]
                at = (m % 3 * 2 + half) * 32
                for u, piece in (
                    (4 * pair + m // 3, jnp.concatenate([a[:, :64], b[:, :64]], axis=1)),
                    (4 * pair + 2 + m // 3, jnp.concatenate([a[:, 64:], b[:, 64:]], axis=1)),
                ):
                    halves[slot] = piece.astype(jnp.float32)
                    for part in range(2):
                        rows = slice(at + 16 * part, at + 16 * part + 16)
                        out[u, rows, :] = halves[slot, pl.ds(part, 16, stride=2), :].astype(jnp.bfloat16)
                    slot = (slot + 1) % SLOTS
        for u in range(4):
            out[4 * pair + u, DATA_ROWS:ROWS, :] = mine[...]


def pack(blocks, mine):
    return pl.pallas_call(
        pack_kernel,
        out_shape=pltpu.VMEM((32, ROWS, 128), jnp.bfloat16),
        in_specs=[VMEM] * 2,
        out_specs=VMEM,
        scratch_shapes=[pltpu.VMEM((SLOTS, 32, 128), jnp.float32)],
        compiler_params=pltpu.CompilerParams(vmem_limit_bytes=LIMIT),
        name="pack",
    )(on_chip(blocks), on_chip(mine))


CHUNK = 256


def combine_kernel(received, points, out, lattice, *tables):
    for k in range(4):
        at = slice(k * 128, k * 128 + 128)
        rows = received[8 * k : 8 * k + 8, DATA_ROWS:ROWS, :].astype(jnp.float32)
        rows = ((rows[0] + rows[1]) + (rows[2] + rows[3])) + ((rows[4] + rows[5]) + (rows[6] + rows[7]))
        lattice[0:3, at] = rows[0:3]
        lattice[3:4, at] = 1.0 / rows[3:4]
    c1, c2, c3 = (math.cos(2.0 * math.pi * i / QGRID) for i in (1, 2, 3))
    low = lax.broadcasted_iota(jnp.int32, (CHUNK, 128), 1) < 64

    for c, table in enumerate(tables):
        for piece in range(CHUNK // 32):
            q = points[c * CHUNK + piece * 32 : c * CHUNK + piece * 32 + 32, :]
            q0, q1, q2 = (jnp.broadcast_to(q[:, d : d + 1], (32, 128)) for d in range(3))
            upper = slice(piece * 32, piece * 32 + 32)
            lower = slice(CHUNK + piece * 32, CHUNK + piece * 32 + 32)
            for k in range(4):
                at = slice(k * 128, k * 128 + 128)
                other = slice(512 + k * 128, 512 + k * 128 + 128)
                turns = q0 * lattice[0:1, at] + q1 * lattice[1:2, at] + q2 * lattice[2:3, at]
                turns = turns.astype(jnp.int32)
                bit0, bit1, bit2, bit3 = ((turns & b) != 0 for b in (1, 2, 4, 8))
                near = jnp.where(bit1, jnp.where(bit0, c3, c2), jnp.where(bit0, c1, 1.0))
                far = jnp.where(bit1, jnp.where(bit0, c1, c2), jnp.where(bit0, c3, 0.0))
                weight = jnp.broadcast_to(lattice[3:4, at], (32, 128))
                sine_weight = jnp.where(bit3, -weight, weight)
                cosine_weight = jnp.where(bit2, -sine_weight, sine_weight)
                cosine = (jnp.where(bit2, far, near) * cosine_weight).astype(jnp.bfloat16)
                sine = (jnp.where(bit2, near, far) * sine_weight).astype(jnp.bfloat16)
                table[upper, at] = cosine
                table[upper, other] = -sine
                table[lower, at] = sine
                table[lower, other] = cosine

        owners = slice(c * CHUNK // 8, (c + 1) * CHUNK // 8)
        for m in range(3):
            columns = jnp.concatenate(
                [
                    jnp.concatenate(
                        [
                            received[:, at : at + 16, :].reshape(512, 128)
                            for at in (m * 64 + half * 32, m * 64 + half * 32 + 16)
                        ],
                        axis=0,
                    )
                    for half in range(2)
                ],
                axis=1,
            )
            product = jnp.dot(table[...], columns, preferred_element_type=jnp.float32)
            rows = slice(m * 8, m * 8 + 8)
            for half in range(2):
                real = product[:CHUNK, 128 * half : 128 * half + 128]
                imag = product[CHUNK:, 128 * half : 128 * half + 128]
                first = jnp.where(low, real, pltpu.roll(imag, 64, 1))
                second = jnp.where(low, pltpu.roll(real, 64, 1), imag)
                out[owners, 2 * half, rows, :] = first.reshape(CHUNK // 8, 8, 128).astype(jnp.bfloat16)
                out[owners, 2 * half + 1, rows, :] = second.reshape(CHUNK // 8, 8, 128).astype(jnp.bfloat16)


def combine(received, points):
    return pl.pallas_call(
        combine_kernel,
        out_shape=pltpu.VMEM((64, 4, 24, 128), jnp.bfloat16),
        in_specs=[VMEM] * 2,
        out_specs=VMEM,
        scratch_shapes=[pltpu.VMEM((8, 512), jnp.float32)]
        + [pltpu.VMEM((2 * CHUNK, 1024), jnp.bfloat16)] * (512 // CHUNK),
        compiler_params=pltpu.CompilerParams(vmem_limit_bytes=LIMIT),
        name="combine",
    )(on_chip(received), on_chip(points))


def rotate_kernel(summed, factors, out, result, sem):
    low = lax.broadcasted_iota(jnp.int32, (8, 128), 1) < 64

    @pl.loop(0, 4)
    def _(e):
        def piece(h, k):
            rows = slice(k % 3 * 8, k % 3 * 8 + 8)
            return summed[h, 0, k // 3, e, rows, :].astype(jnp.float32) + summed[
                h, 1, k // 3, e, rows, :
            ].astype(jnp.float32)

        @pl.loop(0, 4, unroll=4)
        def _(step):
            blocks = (2 * step, 2 * step + 1)
            real, imag = {}, {}
            for i, block in enumerate(blocks):
                for k in range(6):
                    left, right = piece(2 * block, k), piece(2 * block + 1, k)
                    real[i, k] = jnp.where(low, left, pltpu.roll(right, 64, 1))
                    imag[i, k] = jnp.where(low, pltpu.roll(left, 64, 1), right)
            for n in range(6):
                totals = {}
                for k in range(6):
                    vec_real = factors[k * 6 + n]
                    vec_imag = factors[36 + k * 6 + n]
                    for i in range(2):
                        terms = (
                            real[i, k] * vec_real - imag[i, k] * vec_imag,
                            real[i, k] * vec_imag + imag[i, k] * vec_real,
                        )
                        for part in range(2):
                            totals[i, part] = totals[i, part] + terms[part] if k else terms[part]
                for i, block in enumerate(blocks):
                    for part in range(2):
                        at = e * 96 + n * 16 + block * 2 + part
                        result[pl.ds(at, 8, stride=384), :] = totals[i, part]

        for q in range(8):
            at = pl.ds(pl.multiple_of(q * 384 + e * 96, 32), 96)
            pltpu.make_async_copy(result.at[at], out.at[at], sem).start()

    pltpu.make_async_copy(result, out, sem).wait()


def rotate(summed, factors):
    return pl.pallas_call(
        rotate_kernel,
        out_shape=jax.ShapeDtypeStruct((3072, 128), jnp.float32),
        in_specs=[VMEM] * 2,
        out_specs=pl.BlockSpec(memory_space=pltpu.HBM),
        scratch_shapes=[pltpu.VMEM((3072, 128), jnp.float32), pltpu.SemaphoreType.DMA],
        compiler_params=pltpu.CompilerParams(vmem_limit_bytes=LIMIT),
        name="rotate",
    )(on_chip(summed), on_chip(factors))


def per_device(coupling, rp_coords, degeneracy, qpoints, eigvec):
    place = (lax.axis_index(PLANE) % 8).astype(jnp.int32).reshape(1)
    blocks, mine, points, factors = fetch(
        place,
        coupling.reshape(16, 2, 6, 4096).transpose(0, 2, 1, 3),
        rp_coords,
        degeneracy.reshape(1, 16),
        qpoints,
        eigvec.transpose(2, 3, 1, 0),
    )
    message = pack(blocks.reshape(6, 32, 32, 128), mine)
    received = lax.all_to_all(message, PLANE, 0, 0, tiled=True)
    partial = combine(received, points).reshape(256, 24, 128)
    summed = lax.all_to_all(partial, EVERY, 0, 0, tiled=True)
    result = rotate(summed.reshape(16, 2, 2, 4, 24, 128), factors)
    return result.reshape(8, 4, 6, 8, 2, 128).transpose(0, 1, 4, 2, 3, 5).reshape(8, 4, 2, 6, 1024)


def solution(mesh):
    rp = ("y", "x", "zh", "core")
    inner = Mesh(mesh.devices.reshape(4, 4, 2, 2, 4), EVERY)
    return jax.shard_map(
        per_device,
        mesh=inner,
        in_specs=(P(rp, "re", None, None, None), P(None, rp), P(rp), P(), P(rp, None, None, None)),
        out_specs=P(rp, None, None, None, "re"),
        check_vma=False,
    )
```

```python
import math

import jax
import jax.numpy as jnp
from jax import lax
from jax.experimental import pallas as pl
from jax.experimental.pallas import tpu as pltpu
from jax.sharding import Mesh, PartitionSpec as P

QGRID = 16
PLANE = ("y", "x", "core")
EVERY = ("y", "x", "zh", "core", "re")
OWNERS = ("core", "y", "x", "zh", "re")
DATA_ROWS = 192
ROWS = 200


def fetch_kernel(
    place, coupling, coords, degeneracy, qpoints, eigvec,
    blocks, mine, points, rotation,
    coords_in, degeneracy_in, qpoints_in, eigvec_in, rows, columns, sems, small_sems,
):
    small = [
        pltpu.make_async_copy(source, target, small_sems.at[i])
        for i, (source, target) in enumerate(
            [(coords, coords_in), (degeneracy, degeneracy_in), (qpoints, qpoints_in), (eigvec, eigvec_in)]
        )
    ]
    for copy in small:
        copy.start()
    for m in range(6):
        @pl.loop(0, 4)
        def _(group):
            for i in range(8):
                b = group * 8 + i
                pltpu.make_async_copy(
                    coupling.at[:, m, :, pl.ds(pl.multiple_of(b * 128, 128), 128)],
                    blocks.at[m, b],
                    sems.at[m],
                ).start(priority=i % 2)
    for copy in small:
        copy.wait()

    lane = lax.broadcasted_iota(jnp.int32, (16, 128), 1)
    row = lax.broadcasted_iota(jnp.int32, (16, 128), 0)
    spread = (lane == place[0] * 16 + row).astype(jnp.float32).astype(jnp.bfloat16)
    rows[...] = jnp.zeros_like(rows)
    for at, values in ((slice(0, 3), coords_in), (slice(3, 4), degeneracy_in)):
        rows[at, 0:128] = jnp.dot(
            values[...].astype(jnp.float32).astype(jnp.bfloat16), spread, preferred_element_type=jnp.float32
        )
    mine[...] = rows[:, 0:128].astype(jnp.bfloat16)

    rows[...] = jnp.zeros_like(rows)
    rows[0:3, :] = qpoints_in[...].astype(jnp.float32)
    points[...] = jnp.transpose(rows[...])

    columns[...] = jnp.zeros_like(columns)
    for part in range(2):
        for k in range(6):
            for n in range(6):
                i = part * 36 + k * 6 + n
                columns[i : i + 1, 0:8] = eigvec_in[k, n, part : part + 1, :]
    turned = jnp.transpose(columns[...])
    lane = lax.broadcasted_iota(jnp.int32, (8, 128), 1)
    mode = lane // 8
    mode = jnp.where(mode < 6, mode, mode - 6)
    same_point = (lane & 7) == lax.broadcasted_iota(jnp.int32, (8, 128), 0)
    for part in range(2):
        for n in range(6):
            factor = jnp.zeros((8, 128), jnp.float32)
            for k in range(6):
                i = part * 36 + k * 6 + n
                factor = jnp.where(mode == k, jnp.broadcast_to(turned[0:8, i : i + 1], (8, 128)), factor)
            factor = jnp.where(same_point, factor, 0.0)
            for term in range(3):
                rounded = factor.astype(jnp.bfloat16)
                at = term * 96 + part * 48 + n * 8
                rotation[at : at + 8, :] = rounded[:, 0:96]
                factor = factor - rounded.astype(jnp.float32)

    for m in range(6):
        pltpu.make_async_copy(blocks.at[m], blocks.at[m], sems.at[m]).wait()


VMEM = pl.BlockSpec(memory_space=pltpu.VMEM)
LIMIT = 16 * 2**20


def on_chip(x):
    return pltpu.with_memory_space_constraint(x, pltpu.VMEM)


def fetch(place, coupling, coords, degeneracy, qpoints, eigvec):
    hbm = pl.BlockSpec(memory_space=pltpu.HBM)
    return pl.pallas_call(
        fetch_kernel,
        out_shape=(
            pltpu.VMEM((6, 32, 16, 2, 128), jnp.bfloat16),
            pltpu.VMEM((8, 128), jnp.bfloat16),
            pltpu.VMEM((512, 8), jnp.float32),
            pltpu.VMEM((288, 96), jnp.bfloat16),
        ),
        in_specs=[pl.BlockSpec(memory_space=pltpu.SMEM)] + [hbm] * 5,
        out_specs=(VMEM,) * 4,
        scratch_shapes=[
            pltpu.VMEM((3, 16), jnp.int32),
            pltpu.VMEM((1, 16), jnp.int32),
            pltpu.VMEM((3, 512), jnp.int32),
            pltpu.VMEM((6, 6, 2, 8), jnp.float32),
            pltpu.VMEM((8, 512), jnp.float32),
            pltpu.VMEM((128, 128), jnp.float32),
            pltpu.SemaphoreType.DMA((6,)),
            pltpu.SemaphoreType.DMA((4,)),
        ],
        compiler_params=pltpu.CompilerParams(vmem_limit_bytes=LIMIT),
        name="fetch",
    )(place, *(pltpu.with_memory_space_constraint(x, pltpu.HBM) for x in (coupling, coords, degeneracy, qpoints, eigvec)))


SLOTS = 8


def pack_kernel(blocks, mine, out, halves):
    @pl.loop(0, 8, unroll=2)
    def _(pair):
        slot = 0
        for m in range(6):
            for half in range(2):
                a = blocks[m, 16 * half + pair]
                b = blocks[m, 16 * half + 8 + pair]
                at = (m % 3 * 2 + half) * 32
                for u, piece in (
                    (4 * pair + m // 3, jnp.concatenate([a[:, :64], b[:, :64]], axis=1)),
                    (4 * pair + 2 + m // 3, jnp.concatenate([a[:, 64:], b[:, 64:]], axis=1)),
                ):
                    halves[slot] = piece.astype(jnp.float32)
                    for part in range(2):
                        rows = slice(at + 16 * part, at + 16 * part + 16)
                        out[u, rows, :] = halves[slot, pl.ds(part, 16, stride=2), :].astype(jnp.bfloat16)
                    slot = (slot + 1) % SLOTS
        for u in range(4):
            out[4 * pair + u, DATA_ROWS:ROWS, :] = mine[...]


def pack(blocks, mine):
    return pl.pallas_call(
        pack_kernel,
        out_shape=pltpu.VMEM((32, ROWS, 128), jnp.bfloat16),
        in_specs=[VMEM] * 2,
        out_specs=VMEM,
        scratch_shapes=[pltpu.VMEM((SLOTS, 32, 128), jnp.float32)],
        compiler_params=pltpu.CompilerParams(vmem_limit_bytes=LIMIT),
        name="pack",
    )(on_chip(blocks), on_chip(mine))


CHUNK = 256


def combine_kernel(received, points, out, lattice, *tables):
    for k in range(4):
        at = slice(k * 128, k * 128 + 128)
        rows = received[8 * k : 8 * k + 8, DATA_ROWS:ROWS, :].astype(jnp.float32)
        rows = ((rows[0] + rows[1]) + (rows[2] + rows[3])) + ((rows[4] + rows[5]) + (rows[6] + rows[7]))
        lattice[0:3, at] = rows[0:3]
        lattice[3:4, at] = 1.0 / rows[3:4]
    c1, c2, c3 = (math.cos(2.0 * math.pi * i / QGRID) for i in (1, 2, 3))
    low = lax.broadcasted_iota(jnp.int32, (CHUNK, 128), 1) < 64

    for c, table in enumerate(tables):
        for piece in range(CHUNK // 32):
            q = points[c * CHUNK + piece * 32 : c * CHUNK + piece * 32 + 32, :]
            q0, q1, q2 = (jnp.broadcast_to(q[:, d : d + 1], (32, 128)) for d in range(3))
            upper = slice(piece * 32, piece * 32 + 32)
            lower = slice(CHUNK + piece * 32, CHUNK + piece * 32 + 32)
            for k in range(4):
                at = slice(k * 128, k * 128 + 128)
                other = slice(512 + k * 128, 512 + k * 128 + 128)
                turns = q0 * lattice[0:1, at] + q1 * lattice[1:2, at] + q2 * lattice[2:3, at]
                turns = turns.astype(jnp.int32)
                bit0, bit1, bit2, bit3 = ((turns & b) != 0 for b in (1, 2, 4, 8))
                near = jnp.where(bit1, jnp.where(bit0, c3, c2), jnp.where(bit0, c1, 1.0))
                far = jnp.where(bit1, jnp.where(bit0, c1, c2), jnp.where(bit0, c3, 0.0))
                weight = jnp.broadcast_to(lattice[3:4, at], (32, 128))
                sine_weight = jnp.where(bit3, -weight, weight)
                cosine_weight = jnp.where(bit2, -sine_weight, sine_weight)
                cosine = (jnp.where(bit2, far, near) * cosine_weight).astype(jnp.bfloat16)
                sine = (jnp.where(bit2, near, far) * sine_weight).astype(jnp.bfloat16)
                table[upper, at] = cosine
                table[upper, other] = -sine
                table[lower, at] = sine
                table[lower, other] = cosine

        owners = slice(c * CHUNK // 16, (c + 1) * CHUNK // 16)
        for m in range(3):
            columns = jnp.concatenate(
                [
                    jnp.concatenate(
                        [
                            received[:, at : at + 16, :].reshape(512, 128)
                            for at in (m * 64 + half * 32, m * 64 + half * 32 + 16)
                        ],
                        axis=0,
                    )
                    for half in range(2)
                ],
                axis=1,
            )
            product = jnp.dot(table[...], columns, preferred_element_type=jnp.float32)
            rows = slice(m * 8, m * 8 + 8)
            for half in range(2):
                real = product[:CHUNK, 128 * half : 128 * half + 128]
                imag = product[CHUNK:, 128 * half : 128 * half + 128]
                first = jnp.where(low, real, pltpu.roll(imag, 64, 1))
                second = jnp.where(low, pltpu.roll(real, 64, 1), imag)
                for quarter, values in ((2 * half, first), (2 * half + 1, second)):
                    values = values.reshape(CHUNK // 16, 2, 8, 128).astype(jnp.bfloat16)
                    for core in range(2):
                        out[core, owners, quarter, rows, :] = values[:, core]


def combine(received, points):
    return pl.pallas_call(
        combine_kernel,
        out_shape=pltpu.VMEM((2, 32, 4, 24, 128), jnp.bfloat16),
        in_specs=[VMEM] * 2,
        out_specs=VMEM,
        scratch_shapes=[pltpu.VMEM((8, 512), jnp.float32)]
        + [pltpu.VMEM((2 * CHUNK, 1024), jnp.bfloat16)] * (512 // CHUNK),
        compiler_params=pltpu.CompilerParams(vmem_limit_bytes=LIMIT),
        name="combine",
    )(on_chip(received), on_chip(points))


GROUP = 4


def rotate_kernel(summed, rotation, out, result, sem):
    low = lax.broadcasted_iota(jnp.int32, (8, 128), 1) < 64
    sign = jnp.where(low, 1.0, -1.0)
    for e in range(4):
        for group in range(16 // GROUP):
            values = jnp.concatenate(
                [
                    jnp.concatenate(
                        [summed[core, group * GROUP + run, half, e] for half in range(2) for core in range(2)], axis=0
                    )
                    for run in range(GROUP)
                ],
                axis=1,
            )
            product = jnp.dot(rotation[...], values, preferred_element_type=jnp.float32)
            product = product[0:96] + product[96:192] + product[192:288]
            for pair in range(GROUP // 2):
                left = slice(pair * 256, pair * 256 + 128)
                right = slice(pair * 256 + 128, pair * 256 + 256)
                for n in range(6):
                    by_real, by_imag = slice(n * 8, n * 8 + 8), slice(48 + n * 8, 56 + n * 8)
                    a, b = product[by_real, left], product[by_real, right]
                    c, d = product[by_imag, left], product[by_imag, right]
                    real = (jnp.where(low, a, d) - pltpu.roll(jnp.where(low, b, c), 64, 1)) * sign
                    imag = jnp.where(low, c, b) + pltpu.roll(jnp.where(low, d, a), 64, 1)
                    at = e * 96 + n * 16 + (group * GROUP // 2 + pair) * 2
                    result[pl.ds(at, 8, stride=384), :] = real
                    result[pl.ds(at + 1, 8, stride=384), :] = imag
        for q in range(8):
            at = pl.ds(q * 384 + e * 96, 96)
            pltpu.make_async_copy(result.at[at], out.at[at], sem).start()

    pltpu.make_async_copy(result, out, sem).wait()


def rotate(summed, rotation):
    return pl.pallas_call(
        rotate_kernel,
        out_shape=jax.ShapeDtypeStruct((3072, 128), jnp.float32),
        in_specs=[VMEM] * 2,
        out_specs=pl.BlockSpec(memory_space=pltpu.HBM),
        scratch_shapes=[pltpu.VMEM((3072, 128), jnp.float32), pltpu.SemaphoreType.DMA],
        compiler_params=pltpu.CompilerParams(vmem_limit_bytes=LIMIT),
        name="rotate",
    )(on_chip(summed), on_chip(rotation))


def per_device(coupling, rp_coords, degeneracy, qpoints, eigvec):
    place = (lax.axis_index(PLANE) % 8).astype(jnp.int32).reshape(1)
    blocks, mine, points, rotation = fetch(
        place,
        coupling.reshape(16, 2, 6, 4096).transpose(0, 2, 1, 3),
        rp_coords,
        degeneracy.reshape(1, 16),
        qpoints,
        eigvec.transpose(2, 3, 1, 0),
    )
    message = pack(blocks.reshape(6, 32, 32, 128), mine)
    received = lax.all_to_all(message, PLANE, 0, 0, tiled=True)
    partial = combine(received, points).reshape(256, 24, 128)
    summed = lax.all_to_all(partial, OWNERS, 0, 0, tiled=True)
    result = rotate(summed.reshape(2, 16, 2, 4, 24, 128), rotation)
    return result.reshape(8, 4, 6, 8, 2, 128).transpose(0, 1, 4, 2, 3, 5).reshape(8, 4, 2, 6, 1024)


def solution(mesh):
    rp = ("y", "x", "zh", "core")
    inner = Mesh(mesh.devices.reshape(4, 4, 2, 2, 4), EVERY)
    return jax.shard_map(
        per_device,
        mesh=inner,
        in_specs=(P(rp, "re", None, None, None), P(None, rp), P(rp), P(), P(rp, None, None, None)),
        out_specs=P(rp, None, None, None, "re"),
        check_vma=False,
    )
```

```python
import math

import jax
import jax.numpy as jnp
from jax import lax
from jax.experimental import pallas as pl
from jax.experimental.pallas import tpu as pltpu
from jax.sharding import Mesh, PartitionSpec as P

QGRID = 16
PLANE = ("y", "x", "core")
EVERY = ("y", "x", "zh", "core", "re")
OWNERS = ("core", "y", "x", "zh", "re")
DATA_ROWS = 192
ROWS = 200


def fetch_kernel(
    place, coupling, coords, degeneracy, qpoints, eigvec,
    blocks, mine, points, rotation,
    coords_in, degeneracy_in, qpoints_in, eigvec_in, rows, columns, sems, small_sems,
):
    small = [
        pltpu.make_async_copy(source, target, small_sems.at[i])
        for i, (source, target) in enumerate(
            [(coords, coords_in), (degeneracy, degeneracy_in), (qpoints, qpoints_in), (eigvec, eigvec_in)]
        )
    ]
    for copy in small:
        copy.start()
    for m in range(6):
        @pl.loop(0, 4)
        def _(group):
            for i in range(8):
                b = group * 8 + i
                pltpu.make_async_copy(
                    coupling.at[:, m, :, pl.ds(pl.multiple_of(b * 128, 128), 128)],
                    blocks.at[m, b],
                    sems.at[m],
                ).start(priority=i % 2)
    for copy in small:
        copy.wait()

    lane = lax.broadcasted_iota(jnp.int32, (16, 128), 1)
    row = lax.broadcasted_iota(jnp.int32, (16, 128), 0)
    spread = (lane == place[0] * 16 + row).astype(jnp.float32).astype(jnp.bfloat16)
    rows[...] = jnp.zeros_like(rows)
    for at, values in ((slice(0, 3), coords_in), (slice(3, 4), degeneracy_in)):
        rows[at, 0:128] = jnp.dot(
            values[...].astype(jnp.float32).astype(jnp.bfloat16), spread, preferred_element_type=jnp.float32
        )
    mine[...] = rows[:, 0:128].astype(jnp.bfloat16)

    rows[...] = jnp.zeros_like(rows)
    rows[0:3, :] = qpoints_in[...].astype(jnp.float32)
    points[...] = jnp.transpose(rows[...])

    columns[...] = jnp.zeros_like(columns)
    for part in range(2):
        for k in range(6):
            for n in range(6):
                i = part * 36 + k * 6 + n
                columns[i : i + 1, 0:8] = eigvec_in[k, n, part : part + 1, :]
    turned = jnp.transpose(columns[...])
    lane = lax.broadcasted_iota(jnp.int32, (8, 128), 1)
    mode = lane // 8
    mode = jnp.where(mode < 6, mode, mode - 6)
    same_point = (lane & 7) == lax.broadcasted_iota(jnp.int32, (8, 128), 0)
    for part in range(2):
        for n in range(6):
            factor = jnp.zeros((8, 128), jnp.float32)
            for k in range(6):
                i = part * 36 + k * 6 + n
                factor = jnp.where(mode == k, jnp.broadcast_to(turned[0:8, i : i + 1], (8, 128)), factor)
            factor = jnp.where(same_point, factor, 0.0)
            for term in range(3):
                rounded = factor.astype(jnp.bfloat16)
                at = term * 96 + part * 48 + n * 8
                rotation[at : at + 8, :] = rounded[:, 0:96]
                factor = factor - rounded.astype(jnp.float32)

    for m in range(6):
        pltpu.make_async_copy(blocks.at[m], blocks.at[m], sems.at[m]).wait()


VMEM = pl.BlockSpec(memory_space=pltpu.VMEM)
LIMIT = 16 * 2**20


def on_chip(x):
    return pltpu.with_memory_space_constraint(x, pltpu.VMEM)


def fetch(place, coupling, coords, degeneracy, qpoints, eigvec):
    hbm = pl.BlockSpec(memory_space=pltpu.HBM)
    return pl.pallas_call(
        fetch_kernel,
        out_shape=(
            pltpu.VMEM((6, 32, 16, 2, 128), jnp.bfloat16),
            pltpu.VMEM((8, 128), jnp.bfloat16),
            pltpu.VMEM((512, 8), jnp.float32),
            pltpu.VMEM((288, 96), jnp.bfloat16),
        ),
        in_specs=[pl.BlockSpec(memory_space=pltpu.SMEM)] + [hbm] * 5,
        out_specs=(VMEM,) * 4,
        scratch_shapes=[
            pltpu.VMEM((3, 16), jnp.int32),
            pltpu.VMEM((1, 16), jnp.int32),
            pltpu.VMEM((3, 512), jnp.int32),
            pltpu.VMEM((6, 6, 2, 8), jnp.float32),
            pltpu.VMEM((8, 512), jnp.float32),
            pltpu.VMEM((128, 128), jnp.float32),
            pltpu.SemaphoreType.DMA((6,)),
            pltpu.SemaphoreType.DMA((4,)),
        ],
        compiler_params=pltpu.CompilerParams(vmem_limit_bytes=LIMIT),
        name="fetch",
    )(place, *(pltpu.with_memory_space_constraint(x, pltpu.HBM) for x in (coupling, coords, degeneracy, qpoints, eigvec)))


SLOTS = 24


def pack_kernel(blocks, mine, out, halves):
    @pl.loop(0, 8, unroll=8)
    def _(pair):
        slot = 0
        for m in range(6):
            for half in range(2):
                a = blocks[m, 16 * half + pair]
                b = blocks[m, 16 * half + 8 + pair]
                at = (m % 3 * 2 + half) * 32
                for u, piece in (
                    (4 * pair + m // 3, jnp.concatenate([a[:, :64], b[:, :64]], axis=1)),
                    (4 * pair + 2 + m // 3, jnp.concatenate([a[:, 64:], b[:, 64:]], axis=1)),
                ):
                    halves[slot] = piece.astype(jnp.float32)
                    for part in range(2):
                        rows = slice(at + 16 * part, at + 16 * part + 16)
                        out[u, rows, :] = halves[slot, pl.ds(part, 16, stride=2), :].astype(jnp.bfloat16)
                    slot = (slot + 1) % SLOTS
        for u in range(4):
            out[4 * pair + u, DATA_ROWS:ROWS, :] = mine[...]


def pack(blocks, mine):
    return pl.pallas_call(
        pack_kernel,
        out_shape=pltpu.VMEM((32, ROWS, 128), jnp.bfloat16),
        in_specs=[VMEM] * 2,
        out_specs=VMEM,
        scratch_shapes=[pltpu.VMEM((SLOTS, 32, 128), jnp.float32)],
        compiler_params=pltpu.CompilerParams(vmem_limit_bytes=LIMIT),
        name="pack",
    )(on_chip(blocks), on_chip(mine))


CHUNK = 256


def combine_kernel(received, points, out, lattice, *tables):
    for k in range(4):
        at = slice(k * 128, k * 128 + 128)
        rows = received[8 * k : 8 * k + 8, DATA_ROWS:ROWS, :].astype(jnp.float32)
        rows = ((rows[0] + rows[1]) + (rows[2] + rows[3])) + ((rows[4] + rows[5]) + (rows[6] + rows[7]))
        lattice[0:3, at] = rows[0:3]
        lattice[3:4, at] = 1.0 / rows[3:4]
    c1, c2, c3 = (math.cos(2.0 * math.pi * i / QGRID) for i in (1, 2, 3))
    low = lax.broadcasted_iota(jnp.int32, (CHUNK, 128), 1) < 64

    for c, table in enumerate(tables):
        for piece in range(CHUNK // 32):
            q = points[c * CHUNK + piece * 32 : c * CHUNK + piece * 32 + 32, :]
            q0, q1, q2 = (jnp.broadcast_to(q[:, d : d + 1], (32, 128)) for d in range(3))
            upper = slice(piece * 32, piece * 32 + 32)
            lower = slice(CHUNK + piece * 32, CHUNK + piece * 32 + 32)
            for k in range(4):
                at = slice(k * 128, k * 128 + 128)
                other = slice(512 + k * 128, 512 + k * 128 + 128)
                turns = q0 * lattice[0:1, at] + q1 * lattice[1:2, at] + q2 * lattice[2:3, at]
                turns = turns.astype(jnp.int32)
                bit0, bit1, bit2, bit3 = ((turns & b) != 0 for b in (1, 2, 4, 8))
                near = jnp.where(bit1, jnp.where(bit0, c3, c2), jnp.where(bit0, c1, 1.0))
                far = jnp.where(bit1, jnp.where(bit0, c1, c2), jnp.where(bit0, c3, 0.0))
                weight = jnp.broadcast_to(lattice[3:4, at], (32, 128))
                sine_weight = jnp.where(bit3, -weight, weight)
                cosine_weight = jnp.where(bit2, -sine_weight, sine_weight)
                cosine = (jnp.where(bit2, far, near) * cosine_weight).astype(jnp.bfloat16)
                sine = (jnp.where(bit2, near, far) * sine_weight).astype(jnp.bfloat16)
                table[upper, at] = cosine
                table[upper, other] = -sine
                table[lower, at] = sine
                table[lower, other] = cosine

        owners = slice(c * CHUNK // 16, (c + 1) * CHUNK // 16)
        for m in range(3):
            columns = jnp.concatenate(
                [
                    jnp.concatenate(
                        [
                            received[:, at : at + 16, :].reshape(512, 128)
                            for at in (m * 64 + half * 32, m * 64 + half * 32 + 16)
                        ],
                        axis=0,
                    )
                    for half in range(2)
                ],
                axis=1,
            )
            product = jnp.dot(table[...], columns, preferred_element_type=jnp.float32)
            rows = slice(m * 8, m * 8 + 8)
            for half in range(2):
                real = product[:CHUNK, 128 * half : 128 * half + 128]
                imag = product[CHUNK:, 128 * half : 128 * half + 128]
                first = jnp.where(low, real, pltpu.roll(imag, 64, 1))
                second = jnp.where(low, pltpu.roll(real, 64, 1), imag)
                for quarter, values in ((2 * half, first), (2 * half + 1, second)):
                    values = values.reshape(CHUNK // 16, 2, 8, 128).astype(jnp.bfloat16)
                    for core in range(2):
                        out[core, owners, quarter, rows, :] = values[:, core]


def combine(received, points):
    return pl.pallas_call(
        combine_kernel,
        out_shape=pltpu.VMEM((2, 32, 4, 24, 128), jnp.bfloat16),
        in_specs=[VMEM] * 2,
        out_specs=VMEM,
        scratch_shapes=[pltpu.VMEM((8, 512), jnp.float32)]
        + [pltpu.VMEM((2 * CHUNK, 1024), jnp.bfloat16)] * (512 // CHUNK),
        compiler_params=pltpu.CompilerParams(vmem_limit_bytes=LIMIT),
        name="combine",
    )(on_chip(received), on_chip(points))


GROUP = 4


def rotate_kernel(summed, rotation, out, result, sem):
    low = lax.broadcasted_iota(jnp.int32, (8, 128), 1) < 64
    sign = jnp.where(low, 1.0, -1.0)
    for e in range(4):
        for group in range(16 // GROUP):
            values = jnp.concatenate(
                [
                    jnp.concatenate(
                        [summed[core, group * GROUP + run, half, e] for half in range(2) for core in range(2)], axis=0
                    )
                    for run in range(GROUP)
                ],
                axis=1,
            )
            product = jnp.dot(rotation[...], values, preferred_element_type=jnp.float32)
            product = product[0:96] + product[96:192] + product[192:288]
            for pair in range(GROUP // 2):
                left = slice(pair * 256, pair * 256 + 128)
                right = slice(pair * 256 + 128, pair * 256 + 256)
                for n in range(6):
                    by_real, by_imag = slice(n * 8, n * 8 + 8), slice(48 + n * 8, 56 + n * 8)
                    a, b = product[by_real, left], product[by_real, right]
                    c, d = product[by_imag, left], product[by_imag, right]
                    real = (jnp.where(low, a, d) - pltpu.roll(jnp.where(low, b, c), 64, 1)) * sign
                    imag = jnp.where(low, c, b) + pltpu.roll(jnp.where(low, d, a), 64, 1)
                    at = e * 96 + n * 16 + (group * GROUP // 2 + pair) * 2
                    result[pl.ds(at, 8, stride=384), :] = real
                    result[pl.ds(at + 1, 8, stride=384), :] = imag
        for q in range(8):
            at = pl.ds(q * 384 + e * 96, 96)
            pltpu.make_async_copy(result.at[at], out.at[at], sem).start()

    pltpu.make_async_copy(result, out, sem).wait()


def rotate(summed, rotation):
    return pl.pallas_call(
        rotate_kernel,
        out_shape=jax.ShapeDtypeStruct((3072, 128), jnp.float32),
        in_specs=[VMEM] * 2,
        out_specs=pl.BlockSpec(memory_space=pltpu.HBM),
        scratch_shapes=[pltpu.VMEM((3072, 128), jnp.float32), pltpu.SemaphoreType.DMA],
        compiler_params=pltpu.CompilerParams(vmem_limit_bytes=LIMIT),
        name="rotate",
    )(on_chip(summed), on_chip(rotation))


def per_device(coupling, rp_coords, degeneracy, qpoints, eigvec):
    place = (lax.axis_index(PLANE) % 8).astype(jnp.int32).reshape(1)
    blocks, mine, points, rotation = fetch(
        place,
        coupling.reshape(16, 2, 6, 4096).transpose(0, 2, 1, 3),
        rp_coords,
        degeneracy.reshape(1, 16),
        qpoints,
        eigvec.transpose(2, 3, 1, 0),
    )
    message = pack(blocks.reshape(6, 32, 32, 128), mine)
    received = lax.all_to_all(message, PLANE, 0, 0, tiled=True)
    partial = combine(received, points).reshape(256, 24, 128)
    summed = lax.all_to_all(partial, OWNERS, 0, 0, tiled=True)
    result = rotate(summed.reshape(2, 16, 2, 4, 24, 128), rotation)
    return result.reshape(8, 4, 6, 8, 2, 128).transpose(0, 1, 4, 2, 3, 5).reshape(8, 4, 2, 6, 1024)


def solution(mesh):
    rp = ("y", "x", "zh", "core")
    inner = Mesh(mesh.devices.reshape(4, 4, 2, 2, 4), EVERY)
    return jax.shard_map(
        per_device,
        mesh=inner,
        in_specs=(P(rp, "re", None, None, None), P(None, rp), P(rp), P(), P(rp, None, None, None)),
        out_specs=P(rp, None, None, None, "re"),
        check_vma=False,
    )
```

```python
import math

import jax
import jax.numpy as jnp
from jax import lax
from jax.experimental import pallas as pl
from jax.experimental.pallas import tpu as pltpu
from jax.sharding import Mesh, PartitionSpec as P

QGRID = 16
PLANE = ("y", "x", "core")
EVERY = ("y", "x", "zh", "core", "re")
OWNERS = ("core", "y", "x", "zh", "re")
DATA_ROWS = 192
ROWS = 200


def fetch_kernel(
    place, coupling, coords, degeneracy, qpoints, eigvec,
    blocks, mine, points, rotation,
    coords_in, degeneracy_in, qpoints_in, eigvec_in, rows, columns, sems, small_sems,
):
    small = [
        pltpu.make_async_copy(source, target, small_sems.at[i])
        for i, (source, target) in enumerate(
            [(coords, coords_in), (degeneracy, degeneracy_in), (qpoints, qpoints_in), (eigvec, eigvec_in)]
        )
    ]
    for copy in small:
        copy.start()
    for m in range(6):
        @pl.loop(0, 4)
        def _(group):
            for i in range(8):
                b = group * 8 + i
                pltpu.make_async_copy(
                    coupling.at[:, m, :, pl.ds(pl.multiple_of(b * 128, 128), 128)],
                    blocks.at[m, b],
                    sems.at[m],
                ).start(priority=i % 2)
    for copy in small:
        copy.wait()

    lane = lax.broadcasted_iota(jnp.int32, (16, 128), 1)
    row = lax.broadcasted_iota(jnp.int32, (16, 128), 0)
    spread = (lane == place[0] * 16 + row).astype(jnp.float32).astype(jnp.bfloat16)
    rows[...] = jnp.zeros_like(rows)
    for at, values in ((slice(0, 3), coords_in), (slice(3, 4), degeneracy_in)):
        rows[at, 0:128] = jnp.dot(
            values[...].astype(jnp.float32).astype(jnp.bfloat16), spread, preferred_element_type=jnp.float32
        )
    mine[...] = rows[:, 0:128].astype(jnp.bfloat16)

    rows[...] = jnp.zeros_like(rows)
    rows[0:3, :] = qpoints_in[...].astype(jnp.float32)
    points[...] = jnp.transpose(rows[...])

    columns[...] = jnp.zeros_like(columns)
    for part in range(2):
        for k in range(6):
            for n in range(6):
                i = part * 36 + k * 6 + n
                columns[i : i + 1, 0:8] = eigvec_in[k, n, part : part + 1, :]
    turned = jnp.transpose(columns[...])
    lane = lax.broadcasted_iota(jnp.int32, (8, 128), 1)
    mode = lane // 8
    mode = jnp.where(mode < 6, mode, mode - 6)
    same_point = (lane & 7) == lax.broadcasted_iota(jnp.int32, (8, 128), 0)
    for part in range(2):
        for n in range(6):
            factor = jnp.zeros((8, 128), jnp.float32)
            for k in range(6):
                i = part * 36 + k * 6 + n
                factor = jnp.where(mode == k, jnp.broadcast_to(turned[0:8, i : i + 1], (8, 128)), factor)
            factor = jnp.where(same_point, factor, 0.0)
            for term in range(2):
                rounded = factor.astype(jnp.bfloat16)
                at = term * 96 + part * 48 + n * 8
                rotation[at : at + 8, :] = rounded[:, 0:96]
                factor = factor - rounded.astype(jnp.float32)

    for m in range(6):
        pltpu.make_async_copy(blocks.at[m], blocks.at[m], sems.at[m]).wait()


VMEM = pl.BlockSpec(memory_space=pltpu.VMEM)
LIMIT = 16 * 2**20


def on_chip(x):
    return pltpu.with_memory_space_constraint(x, pltpu.VMEM)


def fetch(place, coupling, coords, degeneracy, qpoints, eigvec):
    hbm = pl.BlockSpec(memory_space=pltpu.HBM)
    return pl.pallas_call(
        fetch_kernel,
        out_shape=(
            pltpu.VMEM((6, 32, 16, 2, 128), jnp.bfloat16),
            pltpu.VMEM((8, 128), jnp.bfloat16),
            pltpu.VMEM((512, 8), jnp.float32),
            pltpu.VMEM((192, 96), jnp.bfloat16),
        ),
        in_specs=[pl.BlockSpec(memory_space=pltpu.SMEM)] + [hbm] * 5,
        out_specs=(VMEM,) * 4,
        scratch_shapes=[
            pltpu.VMEM((3, 16), jnp.int32),
            pltpu.VMEM((1, 16), jnp.int32),
            pltpu.VMEM((3, 512), jnp.int32),
            pltpu.VMEM((6, 6, 2, 8), jnp.float32),
            pltpu.VMEM((8, 512), jnp.float32),
            pltpu.VMEM((128, 128), jnp.float32),
            pltpu.SemaphoreType.DMA((6,)),
            pltpu.SemaphoreType.DMA((4,)),
        ],
        compiler_params=pltpu.CompilerParams(vmem_limit_bytes=LIMIT),
        name="fetch",
    )(place, *(pltpu.with_memory_space_constraint(x, pltpu.HBM) for x in (coupling, coords, degeneracy, qpoints, eigvec)))


SLOTS = 24


def pack_kernel(blocks, mine, out, halves):
    @pl.loop(0, 8, unroll=8)
    def _(pair):
        slot = 0
        for m in range(6):
            for half in range(2):
                a = blocks[m, 16 * half + pair]
                b = blocks[m, 16 * half + 8 + pair]
                at = (m % 3 * 2 + half) * 32
                for u, piece in (
                    (4 * pair + m // 3, jnp.concatenate([a[:, :64], b[:, :64]], axis=1)),
                    (4 * pair + 2 + m // 3, jnp.concatenate([a[:, 64:], b[:, 64:]], axis=1)),
                ):
                    halves[slot] = piece.astype(jnp.float32)
                    for part in range(2):
                        rows = slice(at + 16 * part, at + 16 * part + 16)
                        out[u, rows, :] = halves[slot, pl.ds(part, 16, stride=2), :].astype(jnp.bfloat16)
                    slot = (slot + 1) % SLOTS
        for u in range(4):
            out[4 * pair + u, DATA_ROWS:ROWS, :] = mine[...]


def pack(blocks, mine):
    return pl.pallas_call(
        pack_kernel,
        out_shape=pltpu.VMEM((32, ROWS, 128), jnp.bfloat16),
        in_specs=[VMEM] * 2,
        out_specs=VMEM,
        scratch_shapes=[pltpu.VMEM((SLOTS, 32, 128), jnp.float32)],
        compiler_params=pltpu.CompilerParams(vmem_limit_bytes=LIMIT),
        name="pack",
    )(on_chip(blocks), on_chip(mine))


CHUNK = 256


def combine_kernel(received, points, out, lattice, *tables):
    for k in range(4):
        at = slice(k * 128, k * 128 + 128)
        rows = received[8 * k : 8 * k + 8, DATA_ROWS:ROWS, :].astype(jnp.float32)
        rows = ((rows[0] + rows[1]) + (rows[2] + rows[3])) + ((rows[4] + rows[5]) + (rows[6] + rows[7]))
        lattice[0:3, at] = rows[0:3]
        lattice[3:4, at] = 1.0 / rows[3:4]
    c1, c2, c3 = (math.cos(2.0 * math.pi * i / QGRID) for i in (1, 2, 3))
    low = lax.broadcasted_iota(jnp.int32, (CHUNK, 128), 1) < 64

    for c, table in enumerate(tables):
        for piece in range(CHUNK // 32):
            q = points[c * CHUNK + piece * 32 : c * CHUNK + piece * 32 + 32, :]
            q0, q1, q2 = (jnp.broadcast_to(q[:, d : d + 1], (32, 128)) for d in range(3))
            upper = slice(piece * 32, piece * 32 + 32)
            lower = slice(CHUNK + piece * 32, CHUNK + piece * 32 + 32)
            for k in range(4):
                at = slice(k * 128, k * 128 + 128)
                other = slice(512 + k * 128, 512 + k * 128 + 128)
                turns = q0 * lattice[0:1, at] + q1 * lattice[1:2, at] + q2 * lattice[2:3, at]
                turns = turns.astype(jnp.int32)
                bit0, bit1, bit2, bit3 = ((turns & b) != 0 for b in (1, 2, 4, 8))
                near = jnp.where(bit1, jnp.where(bit0, c3, c2), jnp.where(bit0, c1, 1.0))
                far = jnp.where(bit1, jnp.where(bit0, c1, c2), jnp.where(bit0, c3, 0.0))
                weight = jnp.broadcast_to(lattice[3:4, at], (32, 128))
                sine_weight = jnp.where(bit3, -weight, weight)
                cosine_weight = jnp.where(bit2, -sine_weight, sine_weight)
                cosine = (jnp.where(bit2, far, near) * cosine_weight).astype(jnp.bfloat16)
                sine = (jnp.where(bit2, near, far) * sine_weight).astype(jnp.bfloat16)
                table[upper, at] = cosine
                table[upper, other] = -sine
                table[lower, at] = sine
                table[lower, other] = cosine

        owners = slice(c * CHUNK // 16, (c + 1) * CHUNK // 16)
        for m in range(3):
            columns = jnp.concatenate(
                [
                    jnp.concatenate(
                        [
                            received[:, at : at + 16, :].reshape(512, 128)
                            for at in (m * 64 + half * 32, m * 64 + half * 32 + 16)
                        ],
                        axis=0,
                    )
                    for half in range(2)
                ],
                axis=1,
            )
            product = jnp.dot(table[...], columns, preferred_element_type=jnp.float32)
            rows = slice(m * 8, m * 8 + 8)
            for half in range(2):
                real = product[:CHUNK, 128 * half : 128 * half + 128]
                imag = product[CHUNK:, 128 * half : 128 * half + 128]
                first = jnp.where(low, real, pltpu.roll(imag, 64, 1))
                second = jnp.where(low, pltpu.roll(real, 64, 1), imag)
                for quarter, values in ((2 * half, first), (2 * half + 1, second)):
                    values = values.reshape(CHUNK // 16, 2, 8, 128).astype(jnp.bfloat16)
                    for core in range(2):
                        out[core, owners, quarter, rows, :] = values[:, core]


def combine(received, points):
    return pl.pallas_call(
        combine_kernel,
        out_shape=pltpu.VMEM((2, 32, 4, 24, 128), jnp.bfloat16),
        in_specs=[VMEM] * 2,
        out_specs=VMEM,
        scratch_shapes=[pltpu.VMEM((8, 512), jnp.float32)]
        + [pltpu.VMEM((2 * CHUNK, 1024), jnp.bfloat16)] * (512 // CHUNK),
        compiler_params=pltpu.CompilerParams(vmem_limit_bytes=LIMIT),
        name="combine",
    )(on_chip(received), on_chip(points))


GROUP = 4


def rotate_kernel(summed, rotation, out, result, sem):
    low = lax.broadcasted_iota(jnp.int32, (8, 128), 1) < 64
    sign = jnp.where(low, 1.0, -1.0)
    for e in range(4):
        for group in range(16 // GROUP):
            values = jnp.concatenate(
                [
                    jnp.concatenate(
                        [summed[core, group * GROUP + run, half, e] for half in range(2) for core in range(2)], axis=0
                    )
                    for run in range(GROUP)
                ],
                axis=1,
            )
            product = jnp.dot(rotation[...], values, preferred_element_type=jnp.float32)
            product = product[0:96] + product[96:192]
            for pair in range(GROUP // 2):
                left = slice(pair * 256, pair * 256 + 128)
                right = slice(pair * 256 + 128, pair * 256 + 256)
                for n in range(6):
                    by_real, by_imag = slice(n * 8, n * 8 + 8), slice(48 + n * 8, 56 + n * 8)
                    a, b = product[by_real, left], product[by_real, right]
                    c, d = product[by_imag, left], product[by_imag, right]
                    real = (jnp.where(low, a, d) - pltpu.roll(jnp.where(low, b, c), 64, 1)) * sign
                    imag = jnp.where(low, c, b) + pltpu.roll(jnp.where(low, d, a), 64, 1)
                    at = e * 96 + n * 16 + (group * GROUP // 2 + pair) * 2
                    result[pl.ds(at, 8, stride=384), :] = real
                    result[pl.ds(at + 1, 8, stride=384), :] = imag
        for q in range(8):
            at = pl.ds(q * 384 + e * 96, 96)
            pltpu.make_async_copy(result.at[at], out.at[at], sem).start()

    pltpu.make_async_copy(result, out, sem).wait()


def rotate(summed, rotation):
    return pl.pallas_call(
        rotate_kernel,
        out_shape=jax.ShapeDtypeStruct((3072, 128), jnp.float32),
        in_specs=[VMEM] * 2,
        out_specs=pl.BlockSpec(memory_space=pltpu.HBM),
        scratch_shapes=[pltpu.VMEM((3072, 128), jnp.float32), pltpu.SemaphoreType.DMA],
        compiler_params=pltpu.CompilerParams(vmem_limit_bytes=LIMIT),
        name="rotate",
    )(on_chip(summed), on_chip(rotation))


def per_device(coupling, rp_coords, degeneracy, qpoints, eigvec):
    place = (lax.axis_index(PLANE) % 8).astype(jnp.int32).reshape(1)
    blocks, mine, points, rotation = fetch(
        place,
        coupling.reshape(16, 2, 6, 4096).transpose(0, 2, 1, 3),
        rp_coords,
        degeneracy.reshape(1, 16),
        qpoints,
        eigvec.transpose(2, 3, 1, 0),
    )
    message = pack(blocks.reshape(6, 32, 32, 128), mine)
    received = lax.all_to_all(message, PLANE, 0, 0, tiled=True)
    partial = combine(received, points).reshape(256, 24, 128)
    summed = lax.all_to_all(partial, OWNERS, 0, 0, tiled=True)
    result = rotate(summed.reshape(2, 16, 2, 4, 24, 128), rotation)
    return result.reshape(8, 4, 6, 8, 2, 128).transpose(0, 1, 4, 2, 3, 5).reshape(8, 4, 2, 6, 1024)


def solution(mesh):
    rp = ("y", "x", "zh", "core")
    inner = Mesh(mesh.devices.reshape(4, 4, 2, 2, 4), EVERY)
    return jax.shard_map(
        per_device,
        mesh=inner,
        in_specs=(P(rp, "re", None, None, None), P(None, rp), P(rp), P(), P(rp, None, None, None)),
        out_specs=P(rp, None, None, None, "re"),
        check_vma=False,
    )
```
